32 devices in a mesh: dp: 4 (over x, y), sp: 8 (over z, core).
Axes of the slice: x: 2, y: 2, z: 4, core: 2. Of those that a mesh axis runs over, the one named last changes fastest.
Arguments:
- x: bfloat16 [8192, 12288], P(('dp', 'sp')), parts along dimension 0
- gain: bfloat16 [12288], replicated
- wq: bfloat16 [12288, 12288], replicated
- wk: bfloat16 [12288, 12288], replicated
- wv: bfloat16 [12288, 12288], replicated
- wo: bfloat16 [12288, 12288], replicated
Outputs:
- output: bfloat16 [8192, 12288], P(('dp', 'sp')), parts along dimension 0
There are 4 independent parts. The reference program is written for one: setup_inputs(seed, part) draws one part's arguments, and reference() takes and returns one part's arrays. A program takes and returns all parts, laid end to end along the dimension named above; an argument that names none is the same for every part.
All inputs are finite; a program needn't handle non-finite values.
Results may differ from the reference program's by a relative error of at most 0.012.
Values are sent between devices in bfloat16 or wider.
A program may use at most 3 GiB of HBM per device.

```python
import jax
import jax.numpy as jnp
from jax import lax

ROWS = 2048
D = 12288
HEADS = 96
KV_HEADS = 96
HEAD = 128
THETA = 10000


def setup_inputs(seed: int = 0, part: int = 0) -> dict:
    kx, kn, kq, kk, kv, ko = jax.random.split(jax.random.key(seed), 6)

    def weights(key, rows, columns):
        return jax.random.normal(key, (rows, columns), jnp.float32) * rows**-0.5

    drawn = {
        "x": jax.random.normal(jax.random.fold_in(kx, part), (ROWS, D), jnp.float32),
        "gain": 1 + 0.1 * jax.random.normal(kn, (D,), jnp.float32),
        "wq": 2 * weights(kq, D, HEADS * HEAD),
        "wk": 2 * weights(kk, D, KV_HEADS * HEAD),
        "wv": 4 * weights(kv, D, KV_HEADS * HEAD),
        "wo": weights(ko, HEADS * HEAD, D),
    }
    return {k: v.astype(jnp.bfloat16) for k, v in drawn.items()}


def normed(x, gain):
    wide = x.astype(jnp.float32)
    scale = lax.rsqrt(jnp.mean(wide * wide, -1, keepdims=True) + 1e-6)
    return (wide * scale * gain.astype(jnp.float32)).astype(jnp.bfloat16)


def turned(t, place, theta):
    half = t.shape[-1] // 2
    angle = place.astype(jnp.float32)[:, None] * theta ** (-jnp.arange(half, dtype=jnp.float32) / half)
    cos, sin = jnp.cos(angle)[:, None], jnp.sin(angle)[:, None]
    a, b = t[..., :half].astype(jnp.float32), t[..., half:].astype(jnp.float32)
    return jnp.concatenate([a * cos - b * sin, b * cos + a * sin], -1).astype(jnp.bfloat16)


def matmul(a, w):
    return jnp.dot(a, w, preferred_element_type=jnp.float32).astype(jnp.bfloat16)


def einsum(form, a, b):
    return jnp.einsum(form, a.astype(jnp.float32), b.astype(jnp.float32))


def attention(q, k, v):
    scores = einsum("tgsd,ugd->gstu", q, k) * q.shape[-1] ** -0.5
    token = jnp.arange(q.shape[0])
    scores = jnp.where(token[:, None] >= token, scores, -jnp.inf)
    weights = jax.nn.softmax(scores, -1).astype(jnp.bfloat16)
    return einsum("gstu,ugd->tgsd", weights, v).astype(jnp.bfloat16)


def reference(x, gain, wq, wk, wv, wo):
    a, place = normed(x, gain), jnp.arange(ROWS)
    q = turned(matmul(a, wq).reshape(ROWS, HEADS, HEAD), place, THETA).reshape(ROWS, KV_HEADS, -1, HEAD)
    k = turned(matmul(a, wk).reshape(ROWS, KV_HEADS, HEAD), place, THETA)
    v = matmul(a, wv).reshape(ROWS, KV_HEADS, HEAD)
    seen = attention(q, k, v).reshape(ROWS, HEADS * HEAD)
    return (x.astype(jnp.float32) + jnp.dot(seen, wo, preferred_element_type=jnp.float32)).astype(jnp.bfloat16)
```

```python
import functools

import jax
import jax.numpy as jnp
from jax import lax
from jax.experimental import pallas as pl
from jax.experimental.pallas import tpu as pltpu
from jax.sharding import PartitionSpec as P

HEAD = 128
THETA = 10000
HIDDEN = -2e30
NEG = -1e30
LOG2E = 1.4426950408889634
MESH = pl.DeviceIdType.MESH
TN = 256
UN = 2


def _dot(a, b, ca, cb):
    return lax.dot_general(a, b, (((ca,), (cb,)), ((), ())), preferred_element_type=jnp.float32)


def _attend(q, blocks):
    e = HEAD**-0.5 * LOG2E
    scores = []
    for k, _, masked in blocks:
        s = _dot(k, q, 1, 1)
        if masked:
            s = jnp.where(lax.broadcasted_iota(jnp.int32, s.shape, 1) >= lax.broadcasted_iota(jnp.int32, s.shape, 0), s, HIDDEN)
        scores.append(s)
    top = scores[0].max(axis=0, keepdims=True)
    for s in scores[1:]:
        top = jnp.maximum(top, s.max(axis=0, keepdims=True))
    mix = None
    for s, (_, v, _) in zip(scores, blocks):
        p = jnp.exp2((s - top) * e).astype(jnp.bfloat16)
        part = _dot(jnp.concatenate([v.T, jnp.ones((8, v.shape[0]), jnp.bfloat16)], axis=0), p, 1, 0)
        mix = part if mix is None else mix + part
    total = mix[HEAD : HEAD + 1]
    return mix[:HEAD] * (1 / total), top * HEAD**-0.5 + jnp.log(total)


def _rcopy(src, dst, send, recv, device):
    return pltpu.make_async_remote_copy(src_ref=src, dst_ref=dst, send_sem=send, recv_sem=recv, device_id={"sp": device}, device_id_type=MESH)


def _kernel(np_, own, x, gain, wq, wk, wv, wo, tab, y, xo, qkv, rq, rkv, ob, ol, ro, rl, oa,
            A, wb, st, ckv, cq, so, sl, dq, dkv, drkv, dr, drl, of, lf, so2, xt, yst,
            xsem, wsem, stsem, as_s, as_r, xo_s, xo_r, qs, qr, ks, kr, cksem, cqsem, sosem, slsem, os_, or_, ls, lr,
            dqsem, dksem, drksem, drsem, drlsem, so2sem, oas, oar, xtsem, yl, ys, yr):
    chip = 2 * own
    D = A.shape[1]
    half = D // 2
    kinds = D // 2 // np_ // 2
    me = lax.axis_index("sp")
    z, c = me // 2, me % 2
    buddy = me + 1 - 2 * c
    at = lambda chip_: 2 * chip_ + c
    mult = pl.multiple_of

    tiles = 12 * np_

    def wload(t):
        p, i = t // 12, t % 12
        col = mult(c * half + (p * 4 + i % 4) * TN, TN)
        for n, w in enumerate((wq, wk, wv)):
            @pl.when(i // 4 == n)
            def _():
                pltpu.make_async_copy(w.at[:, pl.ds(col, TN)], wb.at[t % 2], wsem.at[t % 2]).start()

    def wwait(slot):
        pltpu.make_async_copy(wq.at[:, pl.ds(0, TN)], wb.at[slot], wsem.at[slot]).wait()

    first = mult(c * own, own)
    load = pltpu.make_async_copy(x, A.at[pl.ds(first, own)], xsem)
    load.start()
    wload(0)
    bar = pltpu.get_barrier_semaphore()
    for n in range(1, 8):
        pl.semaphore_signal(bar, inc=1, device_id={"sp": (me + n) % 8}, device_id_type=MESH)
    load.wait()
    pl.semaphore_wait(bar, 7)
    chunk = own // 4
    R = 32

    def xsend():
        return _rcopy(x, xo, xo_s, xo_r, buddy)

    def asend(j):
        rows = pl.ds(mult(first + j * chunk, chunk), chunk)
        return _rcopy(A.at[rows], A.at[rows], as_s.at[j], as_r.at[j], buddy)

    def arecv(j):
        rows = pl.ds(mult((1 - c) * own + j * chunk, chunk), chunk)
        return _rcopy(A.at[rows], A.at[rows], as_s.at[j], as_r.at[j], buddy)

    def norm(j, _):
        for n in range(chunk // R):
            rows = pl.ds(mult(first + j * chunk + n * R, R), R)
            wide = A[rows, :].astype(jnp.float32)
            scale = lax.rsqrt(jnp.mean(wide * wide, -1, keepdims=True) + 1e-6)
            A[rows, :] = (wide * scale * gain[...]).astype(jnp.bfloat16)

        @pl.when(j > 0)
        def _():
            asend(j - 1).start()
        return 0

    lax.fori_loop(0, 4, norm, 0)
    asend(3).start()
    xsend().start()
    for j in range(4):
        arecv(j).wait_recv()
        asend(j).wait_send()

    def q_send(p, kind):
        return _rcopy(qkv.at[p, 0, kind], rq.at[jnp.maximum(z - 1, 0), p], qs.at[kind, p], qr.at[jnp.maximum(z - 1, 0), p], at(kind))

    def q_extra(p):
        return _rcopy(qkv.at[p, 0, 0], rq.at[0, p], qs.at[2, p], qr.at[0, p], at(2))

    def q_recv(s, p):
        return _rcopy(qkv.at[p, 0, 0], rq.at[s, p], qs.at[0, p], qr.at[s, p], buddy)

    kv_kind = jnp.where(z == 1, 0, 1)

    def kv_send(p):
        return _rcopy(qkv.at[p, pl.ds(1, 2), kv_kind], rkv.at[p], ks.at[p], kr.at[p], at(jnp.where(z == 1, 0, jnp.minimum(z + 1, 3))))

    x_kind = jnp.where(z == 1, 1, 0)
    back = jnp.where(z == 2, 1, 0)

    def o_send(p, s):
        to = at(jnp.where(s == 0, jnp.minimum(z + 1, 3), 1 + s))
        return (_rcopy(ob.at[p, s], ro.at[back, p, x_kind], os_.at[s, p], or_.at[back, p, x_kind], to),
                _rcopy(ol.at[p, s], rl.at[back, p, x_kind], ls.at[s, p], lr.at[back, p, x_kind], to))

    def o_recv(p, r, kind):
        return (_rcopy(ob.at[p, 0], ro.at[r, p, kind], os_.at[0, p], or_.at[r, p, kind], buddy),
                _rcopy(ol.at[p, 0], rl.at[r, p, kind], ls.at[0, p], lr.at[r, p, kind], buddy))

    def when_q_sends(p, kind, act):
        @pl.when(z > kind)
        def _():
            act(q_send(p, kind))
        if kind == 0:
            @pl.when(z == 3)
            def _():
                act(q_extra(p))

    def stage(p, i, slot):
        return pltpu.make_async_copy(st.at[slot], qkv.at[p, i // 4, (i % 4) // 2, pl.ds((i % 2) * 2, 2)], stsem.at[slot])

    def project(p):
        def tile(i, _):
            t = p * 12 + i
            slot = t % 2

            @pl.when(t + 1 < tiles)
            def _():
                wload(t + 1)
            wwait(slot)

            @pl.when(i >= 2)
            def _():
                stage(p, i, slot).wait()
            for kind in range(2):
                @pl.when(i == 3 + 2 * kind)
                def _():
                    when_q_sends(p, kind, lambda d: d.start())
            turn = jnp.where(i < 8, 0, 1)
            rows = min(256, chip)
            for r in range(0, chip, rows):
                acc = jnp.dot(A[r : r + rows, :], wb[slot], preferred_element_type=jnp.float32)
                t32 = acc.astype(jnp.bfloat16).astype(jnp.float32)
                for h in range(2):
                    v = t32[:, h * HEAD : (h + 1) * HEAD]
                    st[slot, h, r : r + rows, :] = (v * tab[turn, 0, r : r + rows, :] + pltpu.roll(v, HEAD // 2, 1) * tab[turn, 1, r : r + rows, :]).astype(jnp.bfloat16)
            stage(p, i, slot).start()
            return 0

        lax.fori_loop(0, 12, tile, 0)
        for s in range(2):
            stage(p, 10 + s, s).wait()

        @pl.when(z < 3)
        def _():
            kv_send(p).start()

    def cross(p):
        def emit(s):
            return (pltpu.make_async_copy(so.at[s], ob.at[p, s], sosem.at[s]), pltpu.make_async_copy(sl.at[s], ol.at[p, s], slsem.at[s]))

        def ship(s):
            for d in emit(s):
                d.wait()
            for d in o_send(p, s):
                d.start()

        def unit(s, n):
            sl[s] = jnp.zeros_like(sl[s])

            def heads(g, _):
                got = []
                for u in range(UN):
                    h = g * UN + u
                    got.append(_attend(cq[s, h], [(ckv[b, 0, h], ckv[b, 1, h], False) for b in range(n)]))
                for u, (o, lse) in enumerate(got):
                    h = g * UN + u
                    so[s, h] = o.astype(jnp.bfloat16)
                    sl[s, pl.ds(h, 1), :] = lse
                return 0

            lax.fori_loop(0, 4 // UN, heads, 0)
            for d in emit(s):
                d.start()

        def q_load(s):
            return pltpu.make_async_copy(rq.at[s, p], cq.at[s], cqsem.at[s])

        def kv_load(b):
            src = qkv.at[p, pl.ds(1, 2), x_kind] if b == 0 else rkv.at[p]
            return pltpu.make_async_copy(src, ckv.at[b], cksem.at[b])

        def need(s):
            q_recv(s, p).wait_recv()
            q_load(s).start()

        @pl.when(z < 3)
        def _():
            kv_load(0).start()

            @pl.when(z != 1)
            def _():
                need(0)

            @pl.when(z < 2)
            def _():
                kv_recv(p)
                kv_load(1).start()
                need(1)
                need(2)
            kv_load(0).wait()

            @pl.when(z != 1)
            def _():
                q_load(0).wait()
                unit(0, 1)

            @pl.when(z == 2)
            def _():
                ship(0)

            @pl.when(z < 2)
            def _():
                kv_load(1).wait()

                def more(s, _):
                    q_load(s).wait()
                    unit(s, 2)

                    @pl.when((s > 1) | (z == 0))
                    def _():
                        ship(s - 1)
                    return 0

                lax.fori_loop(1, 3, more, 0)
                ship(2)

    def kv_recv(p):
        _rcopy(qkv.at[p, pl.ds(1, 2), 0], rkv.at[p], ks.at[p], kr.at[p], buddy).wait_recv()

    def diagonal(p):
        def loads(kind):
            return (pltpu.make_async_copy(qkv.at[p, 0, kind], dq.at[kind], dqsem.at[kind]),
                    pltpu.make_async_copy(qkv.at[p, pl.ds(1, 2), kind], dkv.at[kind], dksem.at[kind]))

        def back_loads(r, kind):
            return (pltpu.make_async_copy(ro.at[r, p, kind], dr.at[r, kind], drsem.at[r, kind]),
                    pltpu.make_async_copy(rl.at[r, p, kind], drl.at[r, kind], drlsem.at[r, kind]))

        more = pltpu.make_async_copy(rkv.at[p], drkv, drksem)

        def came(r, kind):
            return (z >= 2) | ((z == 1) & (kind == 0)) if r == 0 else (z == 3) & (kind == 0)

        for kind in range(2):
            for d in loads(kind):
                d.start()

        @pl.when(z == 3)
        def _():
            kv_recv(p)

        @pl.when(z % 2 == 1)
        def _():
            more.start()

        def result(kind):
            cols = pl.ds(mult(p * 4 * kinds + c * 2 * kinds + kind * kinds, kinds), kinds)
            return cols, pltpu.make_async_copy(so2.at[kind], oa.at[:, cols], so2sem.at[kind])

        def one(kind, _):
            for d in loads(kind):
                d.wait()
            for r in range(2):
                @pl.when(came(r, kind))
                def _():
                    for d in o_recv(p, r, kind):
                        d.wait_recv()
                    for d in back_loads(r, kind):
                        d.start()

            def heads(extra):
                def body(g, _):
                    got = []
                    for u in range(UN):
                        h = g * UN + u
                        for q0 in range(0, chip, own):
                            blocks = [(drkv[0, h], drkv[1, h], False)] if extra else []
                            for k0 in range(0, q0 + own, own):
                                keys = slice(k0, k0 + own)
                                blocks.append((dkv[kind, 0, h, keys, :], dkv[kind, 1, h, keys, :], k0 == q0))
                            got.append((h, q0, _attend(dq[kind, h, q0 : q0 + own, :], blocks)))
                    for h, q0, (o, lse) in got:
                        of[h, :, q0 : q0 + own] = o
                        lf[pl.ds(h, 1), q0 : q0 + own] = lse
                    return 0
                lax.fori_loop(0, 4 // UN, body, 0)

            extra = (z % 2 == 1) & (kind == 1)

            @pl.when(extra)
            def _():
                more.wait()
                heads(True)

            @pl.when(jnp.logical_not(extra))
            def _():
                heads(False)

            for r in range(2):
                @pl.when(came(r, kind))
                def _():
                    for d in back_loads(r, kind):
                        d.wait()

                    def add(h, _):
                        la, lb = lf[pl.ds(h, 1), :], drl[r, kind, pl.ds(h, 1), :]
                        top = jnp.maximum(la, lb)
                        ea, eb = jnp.exp(la - top), jnp.exp(lb - top)
                        inv = 1 / (ea + eb)
                        of[h] = of[h] * (ea * inv) + dr[r, kind, h].astype(jnp.float32) * (eb * inv)
                        lf[pl.ds(h, 1), :] = top + jnp.log(ea + eb)
                        return 0
                    lax.fori_loop(0, 4, add, 0)

            for h in range(4):
                so2[kind, :, h * HEAD : (h + 1) * HEAD] = of[h].T.astype(jnp.bfloat16)
            result(kind)[1].start()
            return 0

        lax.fori_loop(0, 2, one, 0)

        for kind in range(2):
            cols, d = result(kind)
            d.wait()
            oa_send(p, kind).start()

    def oa_send(p, kind):
        cols = pl.ds(mult(p * 4 * kinds + c * 2 * kinds + kind * kinds, kinds), kinds)
        return _rcopy(oa.at[:, cols], oa.at[:, cols], oas.at[p, kind], oar.at[p, kind], buddy)

    def oa_recv(p, kind):
        cols = pl.ds(mult(p * 4 * kinds + (1 - c) * 2 * kinds + kind * kinds, kinds), kinds)
        return _rcopy(oa.at[:, cols], oa.at[:, cols], oas.at[p, kind], oar.at[p, kind], buddy)

    def step(n, _):
        @pl.when(n < np_)
        def _():
            project(n)

        @pl.when((n >= 1) & (n <= np_))
        def _():
            cross(n - 1)

        @pl.when(n >= 2)
        def _():
            diagonal(n - 2)
        return 0

    lax.fori_loop(0, np_ + 2, step, 0)

    def wo_load(t, slot):
        out = []
        for p in range(np_):
            for d in range(2):
                rows = 2 * kinds
                out.append(pltpu.make_async_copy(wo.at[pl.ds(d * half + p * rows, rows), pl.ds(mult(c * half + t * TN, TN), TN)],
                                                 wb.at[slot, pl.ds((p * 2 + d) * rows, rows)], wsem.at[slot]))
        return out

    def x_load(t, slot):
        cols = pl.ds(mult(c * half + t * TN, TN), TN)
        return (pltpu.make_async_copy(x.at[:, cols], xt.at[slot, pl.ds(first, own)], xtsem.at[0, slot]),
                pltpu.make_async_copy(xo.at[:, cols], xt.at[slot, pl.ds(mult((1 - c) * own, own), own)], xtsem.at[1, slot]))

    def y_out(t, slot):
        cols = pl.ds(mult(c * half + t * TN, TN), TN)
        return (pltpu.make_async_copy(yst.at[slot, pl.ds(first, own)], y.at[:, cols], yl.at[slot]),
                _rcopy(yst.at[slot, pl.ds(mult((1 - c) * own, own), own)], y.at[:, cols], ys.at[slot], yr, buddy))

    _rcopy(x, xo, xo_s, xo_r, buddy).wait_recv()
    last = half // TN

    def fetch(t, slot):
        for d in wo_load(t, slot) + list(x_load(t, slot)):
            d.start()

    fetch(0, 0)
    for p in range(np_):
        for kind in range(2):
            oa_recv(p, kind).wait_recv()
    load = pltpu.make_async_copy(oa, A, xsem)
    load.start()
    load.wait()

    def out_tile(t, _):
        slot = t % 2

        @pl.when(t + 1 < last)
        def _():
            fetch(t + 1, 1 - slot)
        wwait(slot)
        for d in x_load(t, slot):
            d.wait()

        @pl.when(t >= 2)
        def _():
            a, b = y_out(t, slot)
            a.wait()
            b.wait_send()
        rows = min(256, chip)
        for r in range(0, chip, rows):
            acc = jnp.dot(A[r : r + rows, :], wb[slot], preferred_element_type=jnp.float32)
            yst[slot, r : r + rows, :] = (xt[slot, r : r + rows, :].astype(jnp.float32) + acc).astype(jnp.bfloat16)
        for d in y_out(t, slot):
            d.start()
        return 0

    lax.fori_loop(0, last, out_tile, 0)
    for s in range(2):
        a, b = y_out(last - 2 + s, (last - 2 + s) % 2)
        a.wait()
        b.wait_send()
    theirs = pl.ds(mult((1 - c) * half, half), half)
    _rcopy(y.at[:, theirs], y.at[:, theirs], ys.at[0], yr, buddy).wait_recv()

    xsend().wait_send()

    def drain(p, _):
        for kind in range(2):
            when_q_sends(p, kind, lambda d: d.wait_send())
            oa_send(p, kind).wait_send()

        @pl.when(z < 3)
        def _():
            kv_send(p).wait_send()

        @pl.when((z == 0) | (z == 2))
        def _():
            for d in o_send(p, 0):
                d.wait_send()

        @pl.when(z < 2)
        def _():
            for s in (1, 2):
                for d in o_send(p, s):
                    d.wait_send()
        return 0

    lax.fori_loop(0, np_, drain, 0)


def solution(mesh):
    def step(x, gain, wq, wk, wv, wo):
        own, d = x.shape
        chip, np_ = 2 * own, d // (2 * 8 * HEAD)
        z = lax.axis_index("sp") // 2
        place = (z * chip + jnp.arange(chip)).astype(jnp.float32)
        half = HEAD // 2
        angle = place[:, None] * THETA ** (-jnp.arange(half, dtype=jnp.float32) / half)
        cos, sin = jnp.cos(angle), jnp.sin(angle)
        turn = jnp.stack([jnp.concatenate([cos, cos], -1), jnp.concatenate([-sin, sin], -1)])
        keep = jnp.stack([jnp.ones((chip, HEAD), jnp.float32), jnp.zeros((chip, HEAD), jnp.float32)])
        tab = jnp.stack([turn, keep])
        bf, f32 = jnp.bfloat16, jnp.float32
        shape = jax.ShapeDtypeStruct
        dma, vmem = pltpu.SemaphoreType.DMA, pltpu.VMEM
        outs = [
            shape((own, d), bf),
            shape((own, d), bf),
            shape((np_, 3, 2, 4, chip, HEAD), bf),
            shape((3, np_, 4, chip, HEAD), bf),
            shape((np_, 2, 4, chip, HEAD), bf),
            shape((np_, 3, 4, HEAD, chip), bf),
            shape((np_, 3, 8, chip), f32),
            shape((2, np_, 2, 4, HEAD, chip), bf),
            shape((2, np_, 2, 8, chip), f32),
            shape((chip, d), bf),
        ]
        scratch = [
            vmem((chip, d), bf),
            vmem((2, d, TN), bf),
            vmem((2, 2, chip, HEAD), bf),
            vmem((2, 2, 4, chip, HEAD), bf),
            vmem((3, 4, chip, HEAD), bf),
            vmem((3, 4, HEAD, chip), bf),
            vmem((3, 8, chip), f32),
            vmem((2, 4, chip, HEAD), bf),
            vmem((2, 2, 4, chip, HEAD), bf),
            vmem((2, 4, chip, HEAD), bf),
            vmem((2, 2, 4, HEAD, chip), bf),
            vmem((2, 2, 8, chip), f32),
            vmem((4, HEAD, chip), f32),
            vmem((8, chip), f32),
            vmem((2, chip, 4 * HEAD), bf),
            vmem((2, chip, TN), bf),
            vmem((2, chip, TN), bf),
            dma, dma((2,)), dma((2,)), dma((4,)), dma((4,)), dma, dma,
            dma((3, np_)), dma((3, np_)), dma((np_,)), dma((np_,)),
            dma((2,)), dma((3,)), dma((3,)), dma((3,)),
            dma((3, np_)), dma((2, np_, 2)), dma((3, np_)), dma((2, np_, 2)),
            dma((2,)), dma((2,)), dma, dma((2, 2)), dma((2, 2)),
            dma((2,)), dma((np_, 2)), dma((np_, 2)),
            dma((2, 2)), dma((2,)), dma((2,)), dma,
        ]
        hbm, here = pl.BlockSpec(memory_space=pl.ANY), pl.BlockSpec(memory_space=pltpu.VMEM)
        flops = 2 * chip * d * d * 2 + 3 * 4 * chip * chip * d
        got = pl.pallas_call(
            functools.partial(_kernel, np_, own),
            out_shape=outs,
            in_specs=[hbm, here, hbm, hbm, hbm, hbm, here],
            out_specs=[hbm] * len(outs),
            scratch_shapes=scratch,
            compiler_params=pltpu.CompilerParams(collective_id=0, has_side_effects=True, vmem_limit_bytes=63 * 2**20),
            cost_estimate=pl.CostEstimate(flops=flops, bytes_accessed=4 * d * d, transcendentals=chip * chip * d // HEAD),
            name="attention_half",
        )(x, gain.astype(f32)[None], wq, wk, wv, wo, tab)
        return got[0]

    tokens, whole = P(("dp", "sp"), None), P(None, None)
    return jax.shard_map(
        step,
        mesh=mesh,
        in_specs=(tokens, P(None), whole, whole, whole, whole),
        out_specs=tokens,
        check_vma=False,
    )
```
